32 devices in a mesh: cache: 8 (over z, x), expert: 4 (over y, core).
Axes of the slice: x: 2, y: 2, z: 4, core: 2. Of those that a mesh axis runs over, the one named last changes fastest.
Arguments:
- query: bfloat16 [512, 2048], P('cache', 'expert'), may hold values from -8 to 8
- new_key: bfloat16 [512, 512], P('cache', 'expert'), may hold values from -8 to 8
- new_value: bfloat16 [512, 512], P('cache', 'expert'), may hold values from -6 to 6
- private_keys: bfloat16 [512, 64, 512], P('cache', None, 'expert'), may hold values from -8 to 8
- private_values: bfloat16 [512, 64, 512], P('cache', None, 'expert'), may hold values from -6 to 6
- private_lengths: int32 [512], P('cache'), may hold values from 1 to 64
- prefix_keys: bfloat16 [16, 1024, 512], P('cache', None, 'expert'), may hold values from -8 to 8
- prefix_values: bfloat16 [16, 1024, 512], P('cache', None, 'expert'), may hold values from -6 to 6
- slot_group: int32 [16], replicated, may hold values from 0 to 15, each once
- group_ids: int32 [512, 1], P('cache'), may hold values from 0 to 15; in each aligned block of 64 rows (0 to 63, 64 to 127, ...) at most 8 rows name the same one
- out_weight: bfloat16 [2048, 4096], P('expert', 'cache'), may hold values from -0.125 to 0.125
- hidden_in: bfloat16 [512, 4096], P(('cache', 'expert')), may hold values from -6 to 6
- norm_gain: float32 [4096], replicated, may hold values from 0.1 to 1.9
- expert_ids: int32 [512, 2], P(('cache', 'expert')), may hold values from 0 to 3, all different within a row; in each aligned block of 16 rows (0 to 15, 16 to 31, ...) at most 16 rows name the same one
- gate_weights: float32 [512, 2], P(('cache', 'expert')), may hold values from 0.1 to 0.9
- w_gate: bfloat16 [4, 4096, 14336], P('expert', None, 'cache'), may hold values from -0.09375 to 0.09375
- w_up: bfloat16 [4, 4096, 14336], P('expert', None, 'cache'), may hold values from -0.09375 to 0.09375
- w_down: bfloat16 [4, 14336, 4096], P('expert', 'cache'), may hold values from -0.046875 to 0.046875
Outputs:
- attention: bfloat16 [512, 2048], P('cache', 'expert')
- layer_out: bfloat16 [512, 4096], P(('cache', 'expert'))
The draws below stay inside these ranges and needn't reach their ends.
Inputs may be any that keep to these rules, and one draw needn't show every extreme that they name: `group_ids`: within each aligned block of 64 requests at most 8 name one group. `slot_group`: each group is held by exactly one slot. `private_lengths`: positions 0 to length - 1 of a request's private cache are live. `expert_ids`: each token names two different experts; among the 16 tokens of one device at most 16 name one expert.
All inputs are finite; a program needn't handle non-finite values.
Results may differ from the reference program's by a relative error of at most 0.0095.
Values may be sent and summed in bfloat16 or wider, within the bound.
A program may use at most 128 MiB of HBM per device.

```python
import math
import jax
import jax.numpy as jnp
import numpy as np
from jax import lax

D = 4096
FF = 14336
HEAD_DIM = 128
QPK = 4
TOP = 2
R_DEV = 64
PRIV = 64
PLEN = 1024
MOSTG = 8
KV_HEADS = 4
HEADS = 16
QW = 2048
KVW = 512
EXPERTS = 4
REQS = 512
TOK_DEV = 16
GROUPS = 16
CAPE = 16
N_CACHE = 8
N_EXPERT = 4


def base(key, shape):
    return jnp.clip(jax.random.normal(key, shape, jnp.float32), -6.0, 6.0)


def draw_query(key, part):
    values = base(jax.random.fold_in(key, 11), (REQS, HEADS * HEAD_DIM))
    return values.astype(jnp.bfloat16)


def draw_new_key(key, part):
    values = base(jax.random.fold_in(key, 12), (REQS, KV_HEADS * HEAD_DIM))
    return values.astype(jnp.bfloat16)


def draw_private_keys(key, part):
    values = base(jax.random.fold_in(key, 13), (REQS, PRIV, KV_HEADS * HEAD_DIM))
    return values.astype(jnp.bfloat16)


def draw_prefix_keys(key, part):
    values = base(jax.random.fold_in(key, 14), (GROUPS, PLEN, KV_HEADS * HEAD_DIM))
    return values.astype(jnp.bfloat16)


def touch_ends(drawn, key, low, largest):
    longest = drawn.shape.index(max(drawn.shape))
    spots = []
    for shift in (0, 1):
        where = [jax.random.randint(jax.random.fold_in(key, axis), (), 0, length) for axis, length in enumerate(drawn.shape)]
        where[longest] = (where[longest] + shift) % drawn.shape[longest]
        spots.append(tuple(where))
    return drawn.at[spots[0]].set(low).at[spots[1]].set(largest)


def level_of(own_key, shape, cuts, least, high):
    def one(position, blocks):
        heights = jax.random.uniform(jax.random.fold_in(jax.random.fold_in(own_key, 6), position), (blocks,), jnp.float32, least / len(cuts), high / len(cuts))
        return jnp.repeat(jnp.exp(heights), shape[position] // blocks).reshape((-1,) + (1,) * (len(shape) - position - 1))

    loudness = one(*cuts[0])
    for cut in cuts[1:]:
        loudness = loudness * one(*cut)
    return loudness


def shared_out(stream_key, own, number, rows, number_of, top, bound, skew):
    sequence = jax.random.permutation(stream_key, number_of)
    packed, usual = shares(number_of, rows * top, bound, skew, True), shares(number_of, rows * top, bound, skew, False)
    places = jnp.arange(number_of)

    def named(sizes, turn):
        used = int((sizes > 0).sum())
        fixed = max(1, used // 4)
        passed = fixed + (places - fixed + turn * (used - fixed)) % max(1, number_of - fixed)
        return jnp.zeros((number_of,), jnp.int32).at[sequence[jnp.where(places < fixed, places, passed)]].set(jnp.asarray(sizes, jnp.int32))

    sizes = jnp.where(number % 4 == 0, named(packed, number // 4), named(usual, number - number // 4 - 1))
    mixed = jax.random.permutation(jax.random.fold_in(own, 3), number_of)
    source_of, receiver = mixed[0:number_of // 2 * 2:2], mixed[1:number_of // 2 * 2:2]
    margin = jnp.minimum(sizes[source_of] - 1, bound - sizes[receiver]) // 2
    margin = jnp.where((source_of == sequence[0]) | (receiver == sequence[0]) | (sizes[receiver] == 0), 0, jnp.maximum(margin, 0))
    passed = jax.random.randint(jax.random.fold_in(own, 4), (number_of // 2,), 0, 1 << 20) % (margin + 1)
    sizes = sizes.at[source_of].add(-passed).at[receiver].add(passed)
    items = jnp.searchsorted(jnp.cumsum(sizes), jnp.arange(rows * top), side="right").astype(jnp.int32)
    table = items.reshape(top, rows).T
    table = table[jax.random.permutation(jax.random.fold_in(own, 1), rows)]
    turn = jax.random.randint(jax.random.fold_in(own, 2), (rows, 1), 0, top)
    return jnp.take_along_axis(table, (jnp.arange(top)[None, :] + turn) % top, axis=1)


def shares(number_of, total, most, lean, full):
    weights = [(1 << 20) // math.isqrt(standing ** lean) + 1 for standing in range(1, number_of + 1)]
    largest = most if full else min(most, max(-(-total // number_of), total * weights[0] // sum(weights)))
    least = 1 if total - largest >= number_of - 1 else 0
    given, rest = [largest] + [least] * (number_of - 1), total - largest - least * (number_of - 1)
    while rest > 0:
        free = [i for i in range(1, number_of) if given[i] < largest] or [i for i in range(1, number_of) if given[i] < most]
        mass, left = sum([weights[i] for i in free]), rest
        for i in free:
            extra = min(most - given[i], max(1, left * weights[i] // mass), rest)
            given[i] = given[i] + extra
            rest = rest - extra
    return np.array(given)


def normal_values(rng, dims, width, most, split=(), kind=jnp.bfloat16):
    drawn = width * jax.random.normal(rng, dims, jnp.float32)
    if split:
        drawn = drawn * level_of(rng, dims, split, -0.22, 0.18)
    return jnp.clip(drawn, -most, most).astype(kind)


def setup_inputs(seed: int = 0) -> dict:
    streams_of = jax.random.split(jax.random.key(seed), 19)
    query = draw_query(jax.random.fold_in(streams_of[18], 71), 0)
    new_key = draw_new_key(jax.random.fold_in(streams_of[18], 71), 0)
    new_value = normal_values(streams_of[2], (REQS, KVW), 1.0, 6.0, ((0, 8), (1, 4)))
    private_keys = draw_private_keys(jax.random.fold_in(streams_of[18], 71), 0)
    private_values = normal_values(streams_of[4], (REQS, PRIV, KVW), 1.0, 6.0, ((0, 8), (2, 4)))
    private_lengths = touch_ends(jax.random.randint(streams_of[5], (REQS,), 1, PRIV + 1), jax.random.fold_in(streams_of[5], 1), 1, PRIV).astype(jnp.int32)
    prefix_keys = draw_prefix_keys(jax.random.fold_in(streams_of[18], 71), 0)
    prefix_values = normal_values(streams_of[7], (GROUPS, PLEN, KVW), 1.0, 6.0, ((0, 8), (2, 4)))
    slot_group = jax.random.permutation(streams_of[8], GROUPS).astype(jnp.int32)
    group_ids_keys = jax.random.split(jax.random.fold_in(streams_of[9], 1), REQS // R_DEV)
    group_ids_turns = jax.random.permutation(jax.random.fold_in(streams_of[9], 3), REQS // R_DEV)
    group_ids = jax.vmap(lambda own, number: shared_out(jax.random.fold_in(streams_of[9], 2), own, number, R_DEV, GROUPS, 1, MOSTG, 2))(group_ids_keys, group_ids_turns).reshape((REQS, 1))
    out_weight = normal_values(streams_of[10], (QW, D), QW ** -0.5, 0.125, ((0, 4), (1, 8)))
    hidden_in = normal_values(streams_of[11], (REQS, D), 1.0, 6.0, ((0, 32),))
    norm_gain = jnp.clip(1.0 + 0.18 * jax.random.normal(streams_of[12], (D,), jnp.float32), 0.1, 1.9)
    expert_ids_keys = jax.random.split(jax.random.fold_in(streams_of[13], 1), REQS // TOK_DEV)
    expert_ids_turns = jax.random.permutation(jax.random.fold_in(streams_of[13], 3), REQS // TOK_DEV)
    expert_ids = jax.vmap(lambda own, number: shared_out(jax.random.fold_in(streams_of[13], 2), own, number, TOK_DEV, EXPERTS, TOP, CAPE, 2))(expert_ids_keys, expert_ids_turns).reshape((REQS, TOP))
    gate_weights = jnp.clip(0.1 + 0.79999997 * jax.random.uniform(streams_of[14], (REQS, TOP), jnp.float32) ** level_of(streams_of[14], (REQS, TOP), ((0, 32),), -0.2, 0.2), 0.1, 0.9)
    w_gate = normal_values(streams_of[15], (EXPERTS, D, FF), D ** -0.5, 0.09375, ((0, 4), (2, 8)))
    w_up = normal_values(streams_of[16], (EXPERTS, D, FF), D ** -0.5, 0.09375, ((0, 4), (2, 8)))
    w_down = normal_values(streams_of[17], (EXPERTS, FF, D), FF ** -0.5, 0.046875, ((0, 4), (1, 8)))
    return dict(query=query, new_key=new_key, new_value=new_value, private_keys=private_keys, private_values=private_values, private_lengths=private_lengths, prefix_keys=prefix_keys, prefix_values=prefix_values, slot_group=slot_group, group_ids=group_ids, out_weight=out_weight, hidden_in=hidden_in, norm_gain=norm_gain, expert_ids=expert_ids, gate_weights=gate_weights, w_gate=w_gate, w_up=w_up, w_down=w_down)


NEG = -1e+30
EPSILON = 1e-05

def reference(query, new_key, new_value, private_keys, private_values, private_lengths, prefix_keys, prefix_values, slot_group, group_ids, out_weight, hidden_in, norm_gain, expert_ids, gate_weights, w_gate, w_up, w_down):
    floats = jnp.float32
    scale = 1.0 / math.sqrt(HEAD_DIM)
    queries = query.astype(floats).reshape(REQS, KV_HEADS, QPK, HEAD_DIM)
    own_keys = private_keys.astype(floats).reshape(REQS, PRIV, KV_HEADS, HEAD_DIM)
    own_values = private_values.astype(floats).reshape(REQS, PRIV, KV_HEADS, HEAD_DIM)
    scores = jnp.einsum('rkqd,rpkd->rkqp', queries, own_keys) * scale
    live = jnp.arange(PRIV, dtype=jnp.int32)[None, :] < private_lengths[:, None]
    live4 = live[:, None, None, :]
    scores = jnp.where(live4, scores, NEG)
    fresh = jnp.einsum('rkqd,rkd->rkq', queries, new_key.astype(floats).reshape(REQS, KV_HEADS, HEAD_DIM)) * scale
    top = jnp.maximum(lax.optimization_barrier(jnp.max(scores, axis=-1)), fresh)
    expo = jnp.where(live4, jnp.exp(scores - top[..., None]), 0.0)
    fresh_expo = jnp.exp(fresh - top)
    total = lax.optimization_barrier(jnp.sum(expo, axis=-1)) + fresh_expo
    weights = lax.optimization_barrier(expo.astype(jnp.bfloat16)).astype(floats)
    fresh_weights = lax.optimization_barrier(fresh_expo.astype(jnp.bfloat16)).astype(floats)
    summed = jnp.einsum('rkqp,rpkd->rkqd', weights, own_values)
    summed = summed + fresh_weights[..., None] * new_value.astype(floats).reshape(REQS, KV_HEADS, 1, HEAD_DIM)
    near_out = summed / total[..., None]
    near_lse = top + jnp.log(total)
    matches = group_ids[:, 0][:, None] == slot_group[None, :]
    slot = lax.optimization_barrier(jnp.sum(jnp.where(matches, jnp.arange(GROUPS, dtype=jnp.int32)[None, :], 0), axis=1)).astype(jnp.int32)
    blocks = REQS // R_DEV

    def prefix_block(items):
        block_queries, block_slots = items
        keys = prefix_keys[block_slots].astype(floats).reshape(-1, PLEN, KV_HEADS, HEAD_DIM)
        values = prefix_values[block_slots].astype(floats).reshape(-1, PLEN, KV_HEADS, HEAD_DIM)
        block_scores = jnp.einsum('rkqd,rpkd->rkqp', block_queries, keys) * scale
        block_top = lax.optimization_barrier(jnp.max(block_scores, axis=-1))
        block_expo = jnp.exp(block_scores - block_top[..., None])
        block_total = lax.optimization_barrier(jnp.sum(block_expo, axis=-1))
        block_weights = lax.optimization_barrier(block_expo.astype(jnp.bfloat16)).astype(floats)
        block_sum = jnp.einsum('rkqp,rpkd->rkqd', block_weights, values)
        return (block_sum / block_total[..., None], block_top + jnp.log(block_total))
    far_out, far_lse = lax.map(prefix_block, (queries.reshape(blocks, R_DEV, KV_HEADS, QPK, HEAD_DIM), slot.reshape(blocks, R_DEV)))
    far_out = far_out.reshape(REQS, KV_HEADS, QPK, HEAD_DIM)
    far_lse = far_lse.reshape(REQS, KV_HEADS, QPK)
    both = jnp.logaddexp(near_lse, far_lse)
    merged = near_out * jnp.exp(near_lse - both)[..., None] + far_out * jnp.exp(far_lse - both)[..., None]
    attention = merged.reshape(REQS, QW).astype(jnp.bfloat16)
    proj = jnp.dot(attention, out_weight, preferred_element_type=jnp.float32)
    resid = hidden_in.astype(floats) + proj
    normed = (resid * lax.rsqrt(lax.optimization_barrier(jnp.mean(resid * resid, axis=-1, keepdims=True)) + EPSILON) * norm_gain).astype(jnp.bfloat16)
    capacity = N_CACHE * N_EXPERT * CAPE

    def one_expert(index):
        hit = expert_ids == index
        chosen = jnp.any(hit, axis=1)
        weight = lax.optimization_barrier(jnp.sum(jnp.where(hit, gate_weights, 0.0), axis=1))
        place = (jnp.cumsum(chosen.astype(jnp.int32)) - 1).astype(jnp.int32)
        target = jnp.where(chosen, place, capacity).astype(jnp.int32)
        rows = jnp.zeros((capacity,), jnp.int32).at[target].set(jnp.arange(REQS, dtype=jnp.int32), mode='drop')
        picked = normed[rows]
        gate = jnp.dot(picked, w_gate[index], preferred_element_type=jnp.float32)
        up = jnp.dot(picked, w_up[index], preferred_element_type=jnp.float32)
        act = (jax.nn.silu(gate) * up).astype(jnp.bfloat16)
        out = jnp.dot(act, w_down[index], preferred_element_type=jnp.float32).astype(jnp.bfloat16)
        back = out[jnp.clip(place, 0, capacity - 1)].astype(floats)
        return weight[:, None] * back
    moe = lax.optimization_barrier(jnp.sum(lax.map(one_expert, jnp.arange(EXPERTS, dtype=jnp.int32)), axis=0))
    layer_out = (resid + moe).astype(jnp.bfloat16)
    return (attention, layer_out)
```

```python
import math

import jax
import jax.numpy as jnp
from jax import lax
from jax.sharding import PartitionSpec as P

MOSTG = 8


NEG = -1e30
EPSILON = 1e-05


def private_partial(queries, keys, values, lengths, new_key, new_value, scale):
    scores = jnp.einsum("rhd,rpd->rhp", queries, keys, preferred_element_type=jnp.float32) * scale
    live = jnp.arange(keys.shape[1], dtype=jnp.int32)[None, :] < lengths[:, None]
    scores = jnp.where(live[:, None, :], scores, NEG)
    fresh = jnp.einsum("rhd,rd->rh", queries, new_key, preferred_element_type=jnp.float32) * scale
    top = jnp.maximum(jnp.max(scores, axis=-1), fresh)
    expo = jnp.where(live[:, None, :], jnp.exp(scores - top[..., None]), 0.0)
    fresh_expo = jnp.exp(fresh - top)
    total = jnp.sum(expo, axis=-1) + fresh_expo
    summed = jnp.einsum(
        "rhp,rpd->rhd", expo.astype(jnp.bfloat16), values, preferred_element_type=jnp.float32
    )
    fresh_weight = lax.optimization_barrier(fresh_expo.astype(jnp.bfloat16)).astype(jnp.float32)
    summed = summed + fresh_weight[..., None] * new_value.astype(jnp.float32)[:, None, :]
    return (summed / total[..., None], top + jnp.log(total))


def prefix_partial(received, prefix_keys, prefix_values, scale):
    rows, heads, width = received.shape
    slots = prefix_keys.shape[0]
    blocks = received.reshape(rows // (slots * MOSTG), slots, MOSTG, heads, width)
    scores = (
        jnp.einsum("cgmhd,gpd->cgmhp", blocks, prefix_keys, preferred_element_type=jnp.float32)
        * scale
    )
    top = jnp.max(scores, axis=-1)
    expo = jnp.exp(scores - top[..., None])
    total = jnp.sum(expo, axis=-1)
    summed = jnp.einsum(
        "cgmhp,gpd->cgmhd",
        expo.astype(jnp.bfloat16),
        prefix_values,
        preferred_element_type=jnp.float32,
    )
    outputs = (summed / total[..., None]).reshape(rows, heads, width)
    return (outputs, (top + jnp.log(total)).reshape(rows, heads))


def split_in_three(values):
    first = lax.reduce_precision(values, 8, 7)
    rest = values - first
    second = lax.reduce_precision(rest, 8, 7)
    third = rest - second
    return jnp.concatenate([first, second, third], axis=1).astype(jnp.bfloat16)


def on_device(
    query,
    new_key,
    new_value,
    private_keys,
    private_values,
    private_lengths,
    prefix_keys,
    prefix_values,
    slot_group,
    group_ids,
    out_weight,
    hidden_in,
    norm_gain,
    expert_ids,
    gate_weights,
    w_gate,
    w_up,
    w_down,
):
    head_dim = new_key.shape[1]
    requests = query.shape[0]
    heads = query.shape[1] // head_dim
    scale = 1.0 / math.sqrt(head_dim)
    queries = query.reshape(requests, heads, head_dim)
    near_out, near_lse = private_partial(
        queries, private_keys, private_values, private_lengths, new_key, new_value, scale
    )
    slot_count = slot_group.shape[0]
    matches = group_ids[:, 0][:, None] == slot_group[None, :]
    slot = jnp.sum(jnp.where(matches, jnp.arange(slot_count, dtype=jnp.int32)[None, :], 0), axis=1)
    order = jnp.arange(requests, dtype=jnp.int32)
    earlier = order[None, :] < order[:, None]
    rank = jnp.sum((slot[:, None] == slot[None, :]) & earlier, axis=1)
    position = slot * MOSTG + rank
    places = jnp.arange(slot_count * MOSTG, dtype=jnp.int32)
    placing = places[:, None] == position[None, :]
    sent = jnp.dot(placing.astype(jnp.bfloat16), query, preferred_element_type=jnp.float32).astype(
        jnp.bfloat16
    )
    sent = sent.reshape(slot_count * MOSTG, heads, head_dim)
    outputs, lse_part = prefix_partial(
        lax.all_to_all(sent, "cache", split_axis=0, concat_axis=0, tiled=True),
        prefix_keys,
        prefix_values,
        scale,
    )
    places_count = slot_count * MOSTG
    parts = split_in_three(lse_part)
    lanes = jnp.pad(parts, ((0, 0), (0, head_dim - parts.shape[1])))
    packet = jnp.concatenate(
        [outputs.astype(jnp.bfloat16).reshape(places_count, heads * head_dim), lanes], axis=1
    )
    back = lax.all_to_all(packet, "cache", split_axis=0, concat_axis=0, tiled=True)
    taken = jnp.dot(
        placing.astype(jnp.bfloat16).T, back, preferred_element_type=jnp.float32
    )
    far_out = taken[:, : heads * head_dim].reshape(requests, heads, head_dim)
    far_lse = jnp.sum(
        taken[:, heads * head_dim : heads * head_dim + 3 * heads].reshape(requests, 3, heads),
        axis=1,
    )
    both = jnp.logaddexp(near_lse, far_lse)
    merged = (
        near_out * jnp.exp(near_lse - both)[..., None]
        + far_out * jnp.exp(far_lse - both)[..., None]
    )
    attention = merged.astype(jnp.bfloat16).reshape(requests, heads * head_dim)
    experts = lax.axis_size("expert")
    tokens = hidden_in.shape[0]
    caches = lax.axis_size("cache")
    copies = jnp.broadcast_to(attention[None], (caches,) + attention.shape)
    every = lax.all_to_all(copies, "cache", split_axis=0, concat_axis=0, tiled=True)
    terms = jnp.dot(
        every.reshape(caches * requests, heads * head_dim),
        out_weight,
        preferred_element_type=jnp.float32,
    ).astype(jnp.bfloat16)
    columns = terms.shape[1]
    regrouped = lax.all_to_all(
        terms.reshape(caches * experts, tokens, columns),
        ("cache", "expert"),
        split_axis=0,
        concat_axis=0,
        tiled=True,
    )
    summed_blocks = jnp.sum(
        regrouped.reshape(caches, experts, tokens, columns).astype(jnp.float32), axis=1
    )
    proj = summed_blocks.transpose(1, 0, 2).reshape(tokens, caches * columns)
    resid = hidden_in.astype(jnp.float32) + proj
    normed = (
        resid * lax.rsqrt(jnp.mean(resid * resid, axis=-1, keepdims=True) + EPSILON) * norm_gain
    ).astype(jnp.bfloat16)
    capacity = max(2, 4 * tokens // experts)
    flat_ids = expert_ids.reshape(-1)
    order_ids = jnp.arange(flat_ids.shape[0], dtype=jnp.int32)
    before = order_ids[None, :] < order_ids[:, None]
    slot_rank = jnp.sum((flat_ids[:, None] == flat_ids[None, :]) & before, axis=1)
    destination = flat_ids * capacity + slot_rank
    expert_slots = jnp.arange(experts * capacity, dtype=jnp.int32)
    chosen = (destination[None, :] == expert_slots[:, None]).reshape(experts * capacity, tokens, 2)
    picking = jnp.sum(chosen.astype(jnp.bfloat16), axis=2)
    outgoing = jnp.dot(picking, normed, preferred_element_type=jnp.float32).astype(jnp.bfloat16)
    arrived = lax.all_to_all(outgoing, "expert", split_axis=0, concat_axis=0, tiled=True)
    half = arrived.shape[0] // 2
    pieces = [
        lax.all_gather(part, "cache", axis=0, tiled=True)
        for part in (arrived[:half], arrived[half:])
    ]
    done = []
    for piece in pieces:
        gate = jnp.dot(piece, w_gate[0], preferred_element_type=jnp.float32)
        up = jnp.dot(piece, w_up[0], preferred_element_type=jnp.float32)
        act = (jax.nn.silu(gate) * up).astype(jnp.bfloat16)
        partial_out = jnp.dot(act, w_down[0], preferred_element_type=jnp.float32)
        done.append(
            lax.psum_scatter(
                partial_out.astype(jnp.bfloat16), "cache", scatter_dimension=0, tiled=True
            )
        )
    summed_rows = jnp.concatenate(done, axis=0)
    returned = lax.all_to_all(summed_rows, "expert", split_axis=0, concat_axis=0, tiled=True)
    mixing = jnp.sum(jnp.where(chosen, gate_weights[None, :, :], 0.0), axis=2)
    moe = jnp.einsum(
        "st,sd->td", mixing, returned.astype(jnp.float32), precision=lax.Precision.HIGHEST
    )
    layer_out = (resid + moe).astype(jnp.bfloat16)
    return (attention, layer_out)


def solution(mesh):
    in_specs = (
        P("cache", "expert"),
        P("cache", "expert"),
        P("cache", "expert"),
        P("cache", None, "expert"),
        P("cache", None, "expert"),
        P("cache"),
        P("cache", None, "expert"),
        P("cache", None, "expert"),
        P(),
        P("cache", None),
        P("expert", "cache"),
        P(("cache", "expert"), None),
        P(),
        P(("cache", "expert"), None),
        P(("cache", "expert"), None),
        P("expert", None, "cache"),
        P("expert", None, "cache"),
        P("expert", "cache", None),
    )
    out_specs = (P("cache", "expert"), P(("cache", "expert"), None))
    return jax.shard_map(
        on_device, mesh=mesh, in_specs=in_specs, out_specs=out_specs, check_vma=False
    )
```
